256 devices in a mesh: gx: 8 (over x, core), gy: 4 (over y), gz: 8 (over z).
Axes of the slice: x: 4, y: 4, z: 8, core: 2. Of those that a mesh axis runs over, the one named last changes fastest.
Arguments:
- velocity: float32 [3, 128, 128, 1024], P(None, 'gx', 'gy', 'gz'), may hold values from -6 to 6
- forcing: float32 [3, 128, 128, 1024], P(None, 'gx', 'gy', 'gz'), may hold values from -12 to 12
- phase_block: int32 [32, 32, 256], P('gx', 'gy', 'gz'), may hold values from 0 to 7
- prefactor: float32 [8], replicated, may hold values from 0.5 to 4
- yield_stress: float32 [8], replicated, may hold values from 1 to 16
Outputs:
- smoothed: float32 [3, 128, 128, 1024], P(None, 'gx', 'gy', 'gz')
- viscosity_field: float32 [128, 128, 1024], P('gx', 'gy', 'gz')
- coarse_one: float32 [64, 64, 512], P('gx', 'gy', 'gz')
- coarse_two: float32 [32, 32, 256], P('gx', 'gy', 'gz')
- coarse_three: float32 [16, 16, 128], P('gx', 'gy', 'gz')
- residual_field: float32 [3, 128, 128, 1024], P(None, 'gx', 'gy', 'gz')
- residual_rms: float32 [], replicated
The draws below stay inside these ranges and needn't reach their ends.
All inputs are finite; a program needn't handle non-finite values.
Results may differ from the reference program's by a relative error of at most 0.000053.
Values sent between devices are 32-bit elements; how exact they have to be, the bound alone decides.
A program may use at most 64 MiB of HBM per device.

```python
import math
import jax
import jax.numpy as jnp
from jax import lax

BLOCK = 4
NPHASE = 8
SWEEPS = 2
NX = 128
NY = 128
NZ = 1024


def draw_forcing(key, part):
    first_key = jax.random.fold_in(key, 11)
    position = jnp.arange(NX, dtype=jnp.float32) / NX
    ramp = (1.0 + 2.0 * position)[None, :, None, None]
    values = jax.random.truncated_normal(first_key, -4.0, 4.0, (3, NX, NY, NZ), jnp.float32)
    return values * ramp


def set_ends(array, stream_key, smallest, high):
    place = [jax.random.randint(jax.random.fold_in(stream_key, axis), (), 0, length) for axis, length in enumerate(array.shape)]
    widest = array.shape.index(max(array.shape))
    beside = place[:widest] + [(place[widest] + 1) % array.shape[widest]] + place[widest + 1:]
    return array.at[tuple(place)].set(smallest).at[tuple(beside)].set(high)


def block_scale(own_key, shape, pieces, smallest, largest):
    def one(dim, parts):
        steps = jax.random.uniform(jax.random.fold_in(jax.random.fold_in(own_key, 6), dim), (parts,), jnp.float32, smallest / len(pieces), largest / len(pieces))
        return jnp.repeat(jnp.exp(steps), shape[dim] // parts).reshape((-1,) + (1,) * (len(shape) - dim - 1))

    loudness = one(*pieces[0])
    for cut in pieces[1:]:
        loudness = loudness * one(*cut)
    return loudness


def bell_draw(own_key, shape, spread, bound, shards=(), kind=jnp.bfloat16):
    values = spread * jax.random.normal(own_key, shape, jnp.float32)
    if shards:
        values = values * block_scale(own_key, shape, shards, -0.22, 0.18)
    return jnp.clip(values, -bound, bound).astype(kind)


def setup_inputs(seed: int = 0) -> dict:
    splits = jax.random.split(jax.random.key(seed), 6)
    velocity = bell_draw(splits[0], (3, NX, NY, NZ), 1.0, 6.0, ((1, 8), (2, 4), (3, 8)), jnp.float32)
    forcing = draw_forcing(jax.random.fold_in(splits[5], 71), 0)
    phase_block = set_ends(jax.random.randint(splits[2], (NX // BLOCK, NY // BLOCK, NZ // BLOCK), 0, NPHASE), jax.random.fold_in(splits[2], 1), 0, NPHASE - 1).astype(jnp.int32)
    prefactor = jnp.clip(jnp.exp(jax.random.uniform(splits[3], (NPHASE,), jnp.float32, math.log(0.5), math.log(4.0))), 0.5, 4.0)
    yield_stress = jnp.clip(jnp.exp(jax.random.uniform(splits[4], (NPHASE,), jnp.float32, math.log(1.0), math.log(16.0))), 1.0, 16.0)
    return dict(velocity=velocity, forcing=forcing, phase_block=phase_block, prefactor=prefactor, yield_stress=yield_stress)


RELAXATION = 0.8
NEIGHBOUR_OFFSETS = ((1, 0, 0), (-1, 0, 0), (0, 1, 0), (0, -1, 0), (0, 0, 1), (0, 0, -1))
UNIT_STEPS = ((1, 0, 0), (0, 1, 0), (0, 0, 1))

def offset_view(field, shift_x, shift_y, shift_z):
    size_x = field.shape[-3] - 2
    size_y = field.shape[-2] - 2
    size_z = field.shape[-1] - 2
    return field[..., 1 + shift_x:1 + shift_x + size_x, 1 + shift_y:1 + shift_y + size_y, 1 + shift_z:1 + shift_z + size_z]

def viscosity_of(padded_vel, prefactor_cells, yield_cells):
    gradient = []
    for comp_a in range(3):
        row_list = []
        for comp_b in range(3):
            step_up = UNIT_STEPS[comp_b]
            step_down = (-step_up[0], -step_up[1], -step_up[2])
            row_list.append(0.5 * (offset_view(padded_vel[comp_a], *step_up) - offset_view(padded_vel[comp_a], *step_down)))
        gradient.append(row_list)
    strain_sq = jnp.zeros(gradient[0][0].shape, jnp.float32)
    for comp_a in range(3):
        for comp_b in range(3):
            strain = 0.5 * (gradient[comp_a][comp_b] + gradient[comp_b][comp_a])
            strain_sq = strain_sq + strain * strain
    invariant = 0.5 * strain_sq + 1.0
    creeping = prefactor_cells * jnp.power(invariant, -1.0 / 3.0)
    plastic = yield_cells / (2.0 * jnp.sqrt(invariant))
    return jnp.minimum(creeping, plastic)

def restrict_dim(field, dim_index):
    coarse_len = (field.shape[dim_index] - 2) // 2

    def every_other(start):
        return lax.slice_in_dim(field, start, start + 2 * coarse_len - 1, 2, dim_index)
    return (every_other(0) + 3.0 * every_other(1) + 3.0 * every_other(2) + every_other(3)) * 0.125

def coarsen(padded):
    return restrict_dim(restrict_dim(restrict_dim(padded, 0), 1), 2)

def smooth_terms(padded_vel, padded_visc):
    centre = offset_view(padded_visc, 0, 0, 0)
    diagonal = jnp.zeros(centre.shape, jnp.float32)
    neighbours = jnp.zeros((3,) + centre.shape, jnp.float32)
    for offset in NEIGHBOUR_OFFSETS:
        face_visc = 0.5 * (centre + offset_view(padded_visc, *offset))
        diagonal = diagonal + face_visc
        neighbours = neighbours + face_visc[None] * offset_view(padded_vel, *offset)
    return (diagonal, neighbours)

def jacobi_sweep(padded_vel, padded_visc, forcing):
    diagonal, neighbours = smooth_terms(padded_vel, padded_visc)
    centre_vel = offset_view(padded_vel, 0, 0, 0)
    return centre_vel + RELAXATION * (forcing - (diagonal[None] * centre_vel - neighbours)) / diagonal[None]

def misfit(padded_vel, padded_visc, forcing):
    diagonal, neighbours = smooth_terms(padded_vel, padded_visc)
    centre_vel = offset_view(padded_vel, 0, 0, 0)
    return forcing - (diagonal[None] * centre_vel - neighbours)

def pad_vel(field):
    return jnp.pad(field, ((0, 0), (1, 1), (1, 1), (1, 1)))

def reference(velocity, forcing, phase_block, prefactor, yield_stress):
    cell_phase = jnp.repeat(jnp.repeat(jnp.repeat(phase_block, BLOCK, 0), BLOCK, 1), BLOCK, 2)
    prefactor_cells = prefactor[cell_phase]
    yield_cells = yield_stress[cell_phase]
    viscosity_field = viscosity_of(pad_vel(velocity), prefactor_cells, yield_cells)
    coarse_one = coarsen(jnp.pad(viscosity_field, 1))
    coarse_two = coarsen(jnp.pad(coarse_one, 1))
    coarse_three = coarsen(jnp.pad(coarse_two, 1))
    padded_visc = jnp.pad(viscosity_field, 1)
    current = velocity
    for sweep_index in range(SWEEPS):
        current = jacobi_sweep(pad_vel(current), padded_visc, forcing)
    misfit_field = misfit(pad_vel(current), padded_visc, forcing)
    residual_rms = jnp.sqrt(jnp.sum(misfit_field * misfit_field) / (3.0 * NX * NY * NZ))
    return (current, viscosity_field, coarse_one, coarse_two, coarse_three, misfit_field, residual_rms)
```

```python
import functools

import jax
import jax.numpy as jnp
import numpy as np
from jax import lax
from jax.experimental import pallas as pl
from jax.experimental.pallas import tpu as pltpu
from jax.sharding import PartitionSpec as P

MESH = pl.DeviceIdType.MESH
RELAX = 0.8
F32 = jnp.float32
G = 4

ROWS = (128, 32, 8)
LANES = ((0, 64), (64, 32), (96, 16))


def depth_operator():
    out = np.zeros((4, 136, 128), np.float32)
    for low_edge in range(2):
        for high_edge in range(2):
            ext = np.eye(128, dtype=np.float64)
            n = 128
            table = out[low_edge * 2 + high_edge]
            first = 0
            for level, (lane, own) in enumerate(LANES):
                n //= 2
                new = np.zeros((n + 2, 128))
                for k in range(-1, n + 1):
                    for offset, weight in ((-1, 1), (0, 3), (1, 3), (2, 1)):
                        i = 2 * k + offset + first
                        if 0 <= i < ext.shape[0]:
                            new[k + 1] += weight / 8 * ext[i]
                if low_edge:
                    new[0] = 0
                if high_edge:
                    new[-1] = 0
                ext, first = new, 1
                table[:128, lane : lane + own] = new[1:-1].T
                table[128 + 2 * level] = new[0]
                table[129 + 2 * level] = new[-1]
    return out


def depth_places():
    sel = np.zeros((16, 128), np.float32)
    for level, (lane, own) in enumerate(LANES):
        sel[1 + 2 * level, lane] = 1
        sel[8 + 2 * level, lane + own - 1] = 1
    return sel


def kernel(
    sizes,
    u_hbm, f_hbm, phase_ref, op_hbm, sel_ref, pref_ref, yield_ref,
    smooth_hbm, visc_hbm, c1_ref, c2_ref, c3_ref, resid_hbm, rms_ref,
    u0, u1, u2, frc, vis, fx, fy, fzl, fzh, rdiag, res,
    cells, yr, ys, zr, zs, vyr, vys, vzr, vzs,
    ap, t1, t2, t3, cxs, cxr, cys, cyr, czs, czr, bc, opm,
    ar_a, ar_b,
    load_sem, out_sem, snd, rcv, vsnd, vrcv, csnd, crcv, asnd, arcv,
):
    nx, ny, nz = sizes
    gx, gy, gz = lax.axis_index("gx"), lax.axis_index("gy"), lax.axis_index("gz")
    coords = {"gx": gx, "gy": gy, "gz": gz}
    has = {
        "gx": (gx > 0, gx < nx - 1),
        "gy": (gy > 0, gy < ny - 1),
        "gz": (gz > 0, gz < nz - 1),
    }
    axes = ("gx", "gy", "gz")

    load_u = pltpu.make_async_copy(u_hbm, u0.at[:, 1:17, 8:40, :], load_sem.at[0])
    load_f = pltpu.make_async_copy(f_hbm, frc, load_sem.at[1])
    edge = (gz == 0).astype(jnp.int32) * 2 + (gz == nz - 1).astype(jnp.int32)
    load_op = pltpu.make_async_copy(op_hbm.at[edge], opm, load_sem.at[2])
    load_u.start()
    load_f.start()
    load_op.start()

    barrier = pltpu.get_barrier_semaphore()

    def greet(i, carry):
        @pl.when(i != gz)
        def _():
            pl.semaphore_signal(barrier, inc=1, device_id={"gz": i}, device_id_type=MESH)
        return carry

    def greet_plane(i, carry):
        px, py = i // ny, i % ny

        @pl.when((px != gx) | (py != gy))
        def _():
            pl.semaphore_signal(barrier, inc=1, device_id={"gx": px, "gy": py}, device_id_type=MESH)
        return carry

    lax.fori_loop(0, nz, greet, 0)
    lax.fori_loop(0, nx * ny, greet_plane, 0)

    lane = lax.broadcasted_iota(jnp.int32, (8, 128), 1)
    lane32 = lax.broadcasted_iota(jnp.int32, (32, 128), 1)

    @pl.when(gx == 0)
    def _():
        zero = jnp.zeros((3, 32, 128), F32)
        for u in (u0, u1, u2):
            u[:, 0, 8:40, :] = zero
        vis[0, 8:40, :] = jnp.zeros((32, 128), F32)
        cxr[0] = jnp.zeros((48, 128), F32)

    @pl.when(gx == nx - 1)
    def _():
        zero = jnp.zeros((3, 32, 128), F32)
        for u in (u0, u1, u2):
            u[:, 17, 8:40, :] = zero
        vis[17, 8:40, :] = jnp.zeros((32, 128), F32)
        cxr[1] = jnp.zeros((48, 128), F32)

    for side, there in enumerate((gy == 0, gy == ny - 1)):
        @pl.when(there)
        def _(side=side):
            for phase in range(3):
                yr[phase, side] = jnp.zeros((3, 16, 128), F32)
            vyr[side] = jnp.zeros((16, 128), F32)
            cyr[side] = jnp.zeros((24, 128), F32)

    for side, there in enumerate((gz == 0, gz == nz - 1)):
        @pl.when(there)
        def _(side=side):
            for phase in range(3):
                zr[phase, side] = jnp.zeros((3, 8, 128), F32)
            vzr[side] = jnp.zeros((8, 128), F32)
            czr[side] = jnp.zeros((8, 256), F32)

    ap[:, 0:8, :] = jnp.zeros((20, 8, 128), F32)
    ap[:, 40:48, :] = jnp.zeros((20, 8, 128), F32)
    t1[...] = jnp.zeros(t1.shape, F32)
    t2[...] = jnp.zeros(t2.shape, F32)

    blocks = phase_ref[...].reshape(32, 32)
    row = lax.broadcasted_iota(jnp.int32, (32, 128), 0)
    spread_z = (lane32 // 4 == row).astype(F32)
    r = lax.broadcasted_iota(jnp.int32, (128, 32), 0)
    c = lax.broadcasted_iota(jnp.int32, (128, 32), 1)
    spread_y = ((r // 32) * 8 + (r % 32) // 4 == c).astype(F32)
    for which, table in enumerate((pref_ref, yield_ref)):
        values = jnp.zeros((32, 32), F32)
        for phase in range(8):
            values = jnp.where(blocks == phase, table[phase], values)
        wide = jnp.dot(values, spread_z, precision=lax.Precision.HIGHEST, preferred_element_type=F32)
        cells[which] = jnp.dot(spread_y, wide, precision=lax.Precision.HIGHEST, preferred_element_type=F32)

    def copies(axis, lo_src, lo_dst, hi_src, hi_dst, send, recv):
        k = axes.index(axis)
        lo = pltpu.make_async_remote_copy(
            lo_src, lo_dst, send.at[k, 0], recv.at[k, 1],
            device_id={axis: coords[axis] - 1}, device_id_type=MESH)
        hi = pltpu.make_async_remote_copy(
            hi_src, hi_dst, send.at[k, 1], recv.at[k, 0],
            device_id={axis: coords[axis] + 1}, device_id_type=MESH)
        return axis, lo, hi

    def start(pair):
        axis, lo, hi = pair

        @pl.when(has[axis][0])
        def _():
            lo.start()

        @pl.when(has[axis][1])
        def _():
            hi.start()

    def wait(pair):
        axis, lo, hi = pair

        @pl.when(has[axis][0])
        def _():
            lo.wait_send()
            hi.wait_recv()

        @pl.when(has[axis][1])
        def _():
            hi.wait_send()
            lo.wait_recv()

    def field_copies(phase, u):
        s, w = snd.at[phase], rcv.at[phase]
        return (
            copies("gz", zs.at[phase], zr.at[phase, 1], zs.at[phase], zr.at[phase, 0], s, w),
            copies("gx", u.at[:, 1, 8:40, :], u.at[:, 17, 8:40, :], u.at[:, 16, 8:40, :], u.at[:, 0, 8:40, :], s, w),
            copies("gy", ys.at[phase, 0], yr.at[phase, 1], ys.at[phase, 1], yr.at[phase, 0], s, w),
        )

    def take_rows(phase, u):
        for comp in range(3):
            for x in range(16):
                u[comp, x + 1, 7:8, :] = yr[phase, 0, comp, x : x + 1, :]
                u[comp, x + 1, 40:41, :] = yr[phase, 1, comp, x : x + 1, :]

    def merged(low, high):
        return jnp.where(lane % 2 == 0, pltpu.roll(high, 127, 1), pltpu.roll(low, 1, 1))

    def ends_of(column, x):
        return jnp.concatenate([pltpu.roll(column, 127 - 8 * x - 2 * t, 1) for t in range(4)], axis=0)

    def packed(acc, plane, x):
        for t in range(4):
            i = 4 * x + t
            acc = jnp.where(lane // 2 == i, pltpu.roll(plane[8 * t : 8 * t + 8], 2 * i + 1, 1), acc)
        return acc

    def along_z(centre, ends):
        up = jnp.where(lane32 == 127, ends, pltpu.roll(centre, 127, 1))
        down = jnp.where(lane32 == 0, ends, pltpu.roll(centre, 1, 1))
        return up, down

    def planes(body, carry):
        def step(i, carry):
            for j in range(G):
                carry = body(i * G + j, carry)
            return carry
        return lax.fori_loop(0, 16 // G, step, carry)

    def pack_rows(phase, comp, x, plane):
        ys[phase, 0, comp, pl.ds(x, 1), :] = plane[0:1]
        ys[phase, 1, comp, pl.ds(x, 1), :] = plane[31:32]

    zero3 = (jnp.zeros((8, 128), F32),) * 3

    load_u.wait()

    def pack_body(x, acc):
        acc = list(acc)
        for comp in range(3):
            plane = u0[comp, x + 1, 8:40, :]
            pack_rows(0, comp, x, plane)
            acc[comp] = packed(acc[comp], plane, x)
        return tuple(acc)

    acc = planes(pack_body, zero3)
    for comp in range(3):
        zs[0, comp] = acc[comp]
    pl.semaphore_wait(barrier, (nz - 1) + (nx * ny - 1))
    sent = field_copies(0, u0)
    for pair in sent:
        start(pair)
    for pair in sent:
        wait(pair)
    take_rows(0, u0)

    def visc_body(x, acc):
        d = []
        for comp in range(3):
            centre = u0[comp, x + 1, 8:40, :]
            up, down = along_z(centre, ends_of(ends[comp], x))
            d.append((
                u0[comp, x + 2, 8:40, :] - u0[comp, x, 8:40, :],
                u0[comp, x + 1, 9:41, :] - u0[comp, x + 1, 7:39, :],
                up - down,
            ))
        diag = d[0][0] * d[0][0] + d[1][1] * d[1][1] + d[2][2] * d[2][2]
        xy, xz, yz = d[0][1] + d[1][0], d[0][2] + d[2][0], d[1][2] + d[2][1]
        off = xy * xy + xz * xz + yz * yz
        inv = diag * 0.125 + off * 0.0625 + 1.0
        block = pl.ds(pl.multiple_of((x // 4) * 32, 32), 32)
        creep = cells[0, block, :] * jnp.exp(jnp.log(inv) * (-1.0 / 3.0))
        plastic = cells[1, block, :] * (0.5 * lax.rsqrt(inv))
        v = jnp.minimum(creep, plastic)
        vis[x + 1, 8:40, :] = v
        vys[0, pl.ds(x, 1), :] = v[0:1]
        vys[1, pl.ds(x, 1), :] = v[31:32]
        return packed(acc, v, x)

    ends = [merged(zr[0, 0, comp], zr[0, 1, comp]) for comp in range(3)]
    vzs[...] = planes(visc_body, jnp.zeros((8, 128), F32))
    vsent = (
        copies("gz", vzs, vzr.at[1], vzs, vzr.at[0], vsnd, vrcv),
        copies("gx", vis.at[1, 8:40, :], vis.at[17, 8:40, :], vis.at[16, 8:40, :], vis.at[0, 8:40, :], vsnd, vrcv),
        copies("gy", vys.at[0], vyr.at[1], vys.at[1], vyr.at[0], vsnd, vrcv),
    )
    for pair in vsent:
        start(pair)
    put_visc = pltpu.make_async_copy(vis.at[1:17, 8:40, :], visc_hbm, out_sem.at[0])
    put_visc.start()

    flag = {a: tuple(jnp.where(h, 1.0, 0.0).astype(F32) for h in has[a]) for a in axes}

    def weighted(get, k, count):
        total = None
        for offset, weight in ((-1, 0.125), (0, 0.375), (1, 0.375), (2, 0.125)):
            i = 2 * k + offset
            if 0 <= i < count:
                term = get(i) * weight
                total = term if total is None else total + term
        return total

    first = 0
    count = 16
    base = 0
    prev = None
    for level, own in enumerate((8, 4, 2)):
        for k in range(-1, own + 1):
            if level == 0:
                value = weighted(lambda i: vis[i + 1, 8:40, :], k, 16)
            else:
                value = None
                for offset, weight in ((-1, 0.125), (0, 0.375), (1, 0.375), (2, 0.125)):
                    i = 2 * k + offset + 1
                    if 0 <= i < prev[1]:
                        term = ap[prev[0] + i, 8:40, :] * weight
                        value = term if value is None else value + term
            if k == -1:
                value = value * flag["gx"][0]
            if k == own:
                value = value * flag["gx"][1]
            ap[base + k + 1, 8:40, :] = value
        prev = (base, own + 2)
        base += own + 2

    def halve(src, start, rows):
        return (
            (src[:, pl.ds(5, rows, stride=2), :] + src[:, pl.ds(8, rows, stride=2), :])
            + 3.0 * (src[:, pl.ds(6, rows, stride=2), :] + src[:, pl.ds(7, rows, stride=2), :])
        ) * 0.125

    low_y, high_y = flag["gy"]
    t1[:, 7:25, :] = halve(ap, 5, 18)
    t1[:, 7:8, :] = t1[:, 7:8, :] * low_y
    t1[:, 24:25, :] = t1[:, 24:25, :] * high_y
    t2[:, 7:17, :] = halve(t1.at[10:20], 5, 10)
    t2[:, 7:8, :] = t2[:, 7:8, :] * low_y
    t2[:, 16:17, :] = t2[:, 16:17, :] * high_y
    t3[:, 7:13, :] = halve(t2.at[6:10], 5, 6)
    t3[:, 7:8, :] = t3[:, 7:8, :] * low_y
    t3[:, 12:13, :] = t3[:, 12:13, :] * high_y

    levels = ((t1, 0, 8, 16, 0, 0), (t2, 0, 4, 8, 24, 8), (t3, 0, 2, 4, 40, 16))
    for t, _, own, rows, at, _ in levels:
        cxs[0, at : at + rows + 2, :] = t[0, 7 : rows + 9, :]
        cxs[1, at : at + rows + 2, :] = t[own + 1, 7 : rows + 9, :]
    cx = copies("gx", cxs.at[0], cxr.at[1], cxs.at[1], cxr.at[0], csnd, crcv)
    start(cx)

    for pair in vsent:
        wait(pair)
    for x in range(16):
        vis[x + 1, 7:8, :] = vyr[0, x : x + 1, :]
        vis[x + 1, 40:41, :] = vyr[1, x : x + 1, :]
    load_f.wait()
    vends = merged(vzr[0], vzr[1])

    def sums(u, column, x, faces):
        centre = u[x + 1, 8:40, :]
        up, down = along_z(centre, ends_of(column, x))
        total = faces[0] * u[x, 8:40, :] + faces[1] * u[x + 2, 8:40, :]
        total = total + (faces[2] * u[x + 1, 7:39, :] + faces[3] * u[x + 1, 9:41, :])
        return centre, total + (faces[4] * down + faces[5] * up)

    def first_body(x, acc):
        centre = vis[x + 1, 8:40, :]
        up, down = along_z(centre, ends_of(vends, x))
        half = 0.5 * centre
        faces = [
            half + 0.5 * vis[x, 8:40, :],
            half + 0.5 * vis[x + 2, 8:40, :],
            half + 0.5 * vis[x + 1, 7:39, :],
            half + 0.5 * vis[x + 1, 9:41, :],
            half + 0.5 * down,
            half + 0.5 * up,
        ]
        fx[x] = faces[0]
        fx[x + 1] = faces[1]
        fy[0, x] = faces[2]
        fy[1, x] = faces[3]
        fzl[x] = faces[4]
        fzh[x] = faces[5]
        diag = ((faces[0] + faces[1]) + (faces[2] + faces[3])) + (faces[4] + faces[5])
        scale = RELAX / diag
        rdiag[0, x] = scale
        rdiag[1, x] = diag
        acc = list(acc)
        for comp in range(3):
            centre, total = sums(u0.at[comp], ends[comp], x, faces)
            new = (1.0 - RELAX) * centre + scale * (frc[comp, x] + total)
            u1[comp, x + 1, 8:40, :] = new
            pack_rows(1, comp, x, new)
            acc[comp] = packed(acc[comp], new, x)
        return tuple(acc)

    def faces_of(x):
        return [fx[x], fx[x + 1], fy[0, x], fy[1, x], fzl[x], fzh[x]]

    acc = planes(first_body, zero3)
    for comp in range(3):
        zs[1, comp] = acc[comp]
    sent = field_copies(1, u1)
    for pair in sent:
        start(pair)

    wait(cx)
    for t, _, own, rows, at, _ in levels:
        t[1, 7 : rows + 9, :] = t[1, 7 : rows + 9, :] + cxr[0, at : at + rows + 2, :]
        t[own, 7 : rows + 9, :] = t[own, 7 : rows + 9, :] + cxr[1, at : at + rows + 2, :]
    for t, _, own, rows, _, at in levels:
        for k in range(own):
            cys[0, at + k : at + k + 1, :] = t[k + 1, 7:8, :]
            cys[1, at + k : at + k + 1, :] = t[k + 1, rows + 8 : rows + 9, :]
    cy = copies("gy", cys.at[0], cyr.at[1], cys.at[1], cyr.at[0], csnd, crcv)
    start(cy)

    for pair in sent:
        wait(pair)
    take_rows(1, u1)
    ends = [merged(zr[1, 0, comp], zr[1, 1, comp]) for comp in range(3)]

    def second_body(x, acc):
        faces = faces_of(x)
        scale = rdiag[0, x]
        acc = list(acc)
        for comp in range(3):
            centre, total = sums(u1.at[comp], ends[comp], x, faces)
            new = (1.0 - RELAX) * centre + scale * (frc[comp, x] + total)
            u2[comp, x + 1, 8:40, :] = new
            pack_rows(2, comp, x, new)
            acc[comp] = packed(acc[comp], new, x)
        return tuple(acc)

    acc = planes(second_body, zero3)
    for comp in range(3):
        zs[2, comp] = acc[comp]
    sent = field_copies(2, u2)
    for pair in sent:
        start(pair)
    put_smooth = pltpu.make_async_copy(u2.at[:, 1:17, 8:40, :], smooth_hbm, out_sem.at[1])
    put_smooth.start()

    wait(cy)
    at = 0
    for t, _, own, rows, _, place in levels:
        for k in range(own):
            value = t[k + 1, 8 : rows + 8, :]
            r = lax.broadcasted_iota(jnp.int32, (rows, 128), 0)
            value = value + jnp.where(r == 0, cyr[0, place + k : place + k + 1, :], 0.0)
            value = value + jnp.where(r == rows - 1, cyr[1, place + k : place + k + 1, :], 0.0)
            bc[at : at + rows, :] = value
            at += rows
    load_op.wait()
    czs[...] = jnp.zeros((8, 256), F32)
    czs[:, 0:168] = lax.dot_general(
        opm[128:136, :], bc[...], (((1,), (1,)), ((), ())),
        precision=lax.Precision.HIGHEST, preferred_element_type=F32)
    cz = copies("gz", czs, czr.at[1], czs, czr.at[0], csnd, crcv)
    start(cz)

    for pair in sent:
        wait(pair)
    take_rows(2, u2)
    ends = [merged(zr[2, 0, comp], zr[2, 1, comp]) for comp in range(3)]

    def resid_body(x, acc):
        faces = faces_of(x)
        diag = rdiag[1, x]
        for comp in range(3):
            centre, total = sums(u2.at[comp], ends[comp], x, faces)
            left = frc[comp, x] + total - diag * centre
            res[comp, x] = left
            square = left * left
            acc = acc + ((square[0:8] + square[8:16]) + (square[16:24] + square[24:32]))
        return acc

    acc = planes(resid_body, jnp.zeros((8, 128), F32))

    ar_a[gz] = jnp.sum(acc, axis=0, keepdims=True)

    def row_copy(i):
        return pltpu.make_async_remote_copy(
            ar_a.at[gz], ar_a.at[gz], asnd.at[0], arcv.at[0], device_id={"gz": i}, device_id_type=MESH)

    def send_row(i, carry):
        @pl.when(i != gz)
        def _():
            row_copy(i).start()
        return carry

    lax.fori_loop(0, nz, send_row, 0)
    put_res = pltpu.make_async_copy(res, resid_hbm, out_sem.at[2])
    put_res.start()

    wait(cz)
    got = jnp.concatenate([czr[0], czr[1]], axis=0)[:, 0:168]
    coarse = jnp.dot(bc[...], opm[0:128, :], precision=lax.Precision.HIGHEST, preferred_element_type=F32)
    coarse = coarse + lax.dot_general(
        got, sel_ref[...], (((0,), (0,)), ((), ())),
        precision=lax.Precision.HIGHEST, preferred_element_type=F32)
    c1_ref[...] = coarse[0:128, 0:64].reshape(8, 16, 64)
    c2_ref[...] = coarse[128:160, 64:96].reshape(4, 8, 32)
    c3_ref[0] = coarse[160:164, 96:112]
    c3_ref[1] = coarse[164:168, 96:112]

    def whole(buf, n, sem):
        return pltpu.make_async_copy(buf.at[0:n], buf.at[0:n], sem)

    whole(ar_a, nz - 1, asnd.at[0]).wait()
    whole(ar_a, nz - 1, arcv.at[0]).wait()
    mine = gx * ny + gy
    line = ar_a[0]
    for i in range(1, nz):
        line = line + ar_a[i]
    ar_b[mine] = line

    def send_plane(i, carry):
        px, py = i // ny, i % ny

        @pl.when((px != gx) | (py != gy))
        def _():
            pltpu.make_async_remote_copy(
                ar_b.at[mine], ar_b.at[mine], asnd.at[1], arcv.at[1],
                device_id={"gx": px, "gy": py}, device_id_type=MESH).start()
        return carry

    lax.fori_loop(0, nx * ny, send_plane, 0)
    put_visc.wait()
    put_smooth.wait()
    put_res.wait()
    whole(ar_b, nx * ny - 1, asnd.at[1]).wait()
    whole(ar_b, nx * ny - 1, arcv.at[1]).wait()
    total = jnp.sum(ar_b[...], axis=0)
    cells_all = float(3 * 16 * nx * 32 * ny * 128 * nz)
    rms_ref[...] = jnp.sqrt(jnp.sum(total, axis=1, keepdims=True) / cells_all)


def per_device(sizes, velocity, forcing, phase_block, prefactor, yield_stress):
    nx, ny, nz = sizes
    vm = lambda *shape: pltpu.VMEM(shape, F32)
    any_, vmem, smem = (pl.BlockSpec(memory_space=s) for s in (pl.ANY, pltpu.VMEM, pltpu.SMEM))
    shape = lambda *s: jax.ShapeDtypeStruct(s, F32)
    out = pl.pallas_call(
        functools.partial(kernel, sizes),
        out_shape=(
            shape(3, 16, 32, 128), shape(16, 32, 128), shape(8, 16, 64), shape(4, 8, 32), shape(2, 4, 16),
            shape(3, 16, 32, 128), shape(1, 1),
        ),
        in_specs=[any_, any_, vmem, any_, vmem, smem, smem],
        out_specs=(any_, any_, vmem, vmem, vmem, any_, vmem),
        scratch_shapes=[
            vm(3, 18, 48, 128), vm(3, 18, 48, 128), vm(3, 18, 48, 128), vm(3, 16, 32, 128), vm(18, 48, 128),
            vm(17, 32, 128), vm(2, 16, 32, 128), vm(16, 32, 128), vm(16, 32, 128), vm(2, 16, 32, 128), vm(3, 16, 32, 128),
            vm(2, 128, 128), vm(3, 2, 3, 16, 128), vm(3, 2, 3, 16, 128), vm(3, 2, 3, 8, 128), vm(3, 3, 8, 128),
            vm(2, 16, 128), vm(2, 16, 128), vm(2, 8, 128), vm(8, 128),
            vm(20, 48, 128), vm(20, 32, 128), vm(10, 24, 128), vm(4, 16, 128),
            vm(2, 48, 128), vm(2, 48, 128), vm(2, 24, 128), vm(2, 24, 128), vm(8, 256), vm(2, 8, 256),
            vm(168, 128), vm(136, 128),
            vm(nz, 1, 128), vm(nx * ny, 1, 128),
            pltpu.SemaphoreType.DMA((3,)), pltpu.SemaphoreType.DMA((3,)),
            pltpu.SemaphoreType.DMA((3, 3, 2)), pltpu.SemaphoreType.DMA((3, 3, 2)),
            pltpu.SemaphoreType.DMA((3, 2)), pltpu.SemaphoreType.DMA((3, 2)),
            pltpu.SemaphoreType.DMA((3, 2)), pltpu.SemaphoreType.DMA((3, 2)),
            pltpu.SemaphoreType.DMA((2,)), pltpu.SemaphoreType.DMA((2,)),
        ],
        compiler_params=pltpu.CompilerParams(collective_id=0, has_side_effects=True),
        name="picard",
    )(
        velocity, forcing, phase_block, jnp.asarray(depth_operator()), jnp.asarray(depth_places()),
        prefactor, yield_stress,
    )
    return out[:6] + (out[6].reshape(()),)


def solution(mesh):
    sizes = tuple(mesh.shape[a] for a in ("gx", "gy", "gz"))
    return jax.shard_map(
        functools.partial(per_device, sizes),
        mesh=mesh,
        in_specs=(P(None, "gx", "gy", "gz"), P(None, "gx", "gy", "gz"), P("gx", "gy", "gz"), P(), P()),
        out_specs=(
            P(None, "gx", "gy", "gz"), P("gx", "gy", "gz"), P("gx", "gy", "gz"), P("gx", "gy", "gz"),
            P("gx", "gy", "gz"), P(None, "gx", "gy", "gz"), P(),
        ),
        check_vma=False,
    )
```

```python
import functools

import jax
import jax.numpy as jnp
import numpy as np
from jax import lax
from jax.experimental import pallas as pl
from jax.experimental.pallas import tpu as pltpu
from jax.sharding import PartitionSpec as P

MESH = pl.DeviceIdType.MESH
RELAX = 0.8
F32 = jnp.float32
VG, LG, SG = 7, 7, 7

ROWS = (128, 32, 8)
LANES = ((0, 64), (64, 32), (96, 16))


def depth_operator():
    out = np.zeros((4, 136, 128), np.float32)
    for low_edge in range(2):
        for high_edge in range(2):
            ext = np.eye(128, dtype=np.float64)
            n = 128
            table = out[low_edge * 2 + high_edge]
            first = 0
            for level, (lane, own) in enumerate(LANES):
                n //= 2
                new = np.zeros((n + 2, 128))
                for k in range(-1, n + 1):
                    for offset, weight in ((-1, 1), (0, 3), (1, 3), (2, 1)):
                        i = 2 * k + offset + first
                        if 0 <= i < ext.shape[0]:
                            new[k + 1] += weight / 8 * ext[i]
                if low_edge:
                    new[0] = 0
                if high_edge:
                    new[-1] = 0
                ext, first = new, 1
                table[:128, lane : lane + own] = new[1:-1].T
                table[128 + 2 * level] = new[0]
                table[129 + 2 * level] = new[-1]
    return out


def depth_places():
    sel = np.zeros((16, 128), np.float32)
    for level, (lane, own) in enumerate(LANES):
        sel[1 + 2 * level, lane] = 1
        sel[8 + 2 * level, lane + own - 1] = 1
    return sel


def kernel(
    sizes,
    u_hbm, f_hbm, phase_hbm, op_hbm, sel_hbm, pref_hbm, yield_hbm,
    u2, vis, c1_ref, c2_ref, c3_ref, res, rms_ref,
    u0, u1, frc, fx, fy, fzl, fzh, fze, diag, scale, base, sx, sy, sz,
    cells, xr, yr, ys, zr, zs, vxr, vyr, vys, vzr, vzs,
    ap, t1, t2, t3, cxs, cxr, cys, cyr, czs, czr, bc, opm,
    ar_a, ar_b, phase_ref, sel_ref, pref_ref, yield_ref,
    load_sem, snd, rcv, vsnd, vrcv, csnd, crcv, asnd, arcv,
):
    nx, ny, nz = sizes
    gx, gy, gz = lax.axis_index("gx"), lax.axis_index("gy"), lax.axis_index("gz")
    coords = {"gx": gx, "gy": gy, "gz": gz}
    has = {
        "gx": (gx > 0, gx < nx - 1),
        "gy": (gy > 0, gy < ny - 1),
        "gz": (gz > 0, gz < nz - 1),
    }
    axes = ("gx", "gy", "gz")

    load_u = pltpu.make_async_copy(u_hbm, u0.at[:, 1:17, 8:40, :], load_sem.at[0])
    load_f = pltpu.make_async_copy(f_hbm, frc, load_sem.at[1])
    edge = (gz == 0).astype(jnp.int32) * 2 + (gz == nz - 1).astype(jnp.int32)
    load_op = pltpu.make_async_copy(op_hbm.at[edge], opm, load_sem.at[2])
    load_phase = pltpu.make_async_copy(phase_hbm, phase_ref, load_sem.at[3])
    load_sel = pltpu.make_async_copy(sel_hbm, sel_ref, load_sem.at[4])
    load_pref = pltpu.make_async_copy(pref_hbm, pref_ref, load_sem.at[5])
    load_yield = pltpu.make_async_copy(yield_hbm, yield_ref, load_sem.at[6])
    for load in (load_u, load_phase, load_pref, load_yield, load_f, load_op, load_sel):
        load.start()

    barrier = pltpu.get_barrier_semaphore()

    core, chip = gx % 2, gx // 2
    beside = gx + 1 - 2 * core
    across = gx - 1 + 2 * core
    has_across = (across >= 0) & (across < nx)
    lines = [(gx, (gz + d) % nz) for d in range(1, nz)] + [(beside, (gz + d) % nz) for d in range(nz)]
    plane = [
        (2 * ((chip + dx) % (nx // 2)) + core, (gy + dy) % ny)
        for dx in range(nx // 2) for dy in range(ny) if (dx, dy) != (0, 0)
    ]

    def greet(**there):
        pl.semaphore_signal(barrier, inc=1, device_id=there, device_id_type=MESH)

    @pl.when(has_across)
    def _():
        greet(gx=across)

    for px, pz in lines:
        greet(gx=px, gz=pz)
    for px, py in plane:
        greet(gx=px, gy=py)

    lane = lax.broadcasted_iota(jnp.int32, (8, 128), 1)
    lane32 = lax.broadcasted_iota(jnp.int32, (32, 128), 1)
    sub8 = lax.broadcasted_iota(jnp.int32, (8, 128), 0)

    def copies(axis, lo_src, lo_dst, hi_src, hi_dst, send, recv):
        k = axes.index(axis)
        lo = pltpu.make_async_remote_copy(
            lo_src, lo_dst, send.at[k, 0], recv.at[k, 1],
            device_id={axis: coords[axis] - 1}, device_id_type=MESH)
        hi = pltpu.make_async_remote_copy(
            hi_src, hi_dst, send.at[k, 1], recv.at[k, 0],
            device_id={axis: coords[axis] + 1}, device_id_type=MESH)
        return axis, lo, hi

    def start(pair):
        axis, lo, hi = pair

        @pl.when(has[axis][0])
        def _():
            lo.start()

        @pl.when(has[axis][1])
        def _():
            hi.start()

    def wait(pair):
        axis, lo, hi = pair

        @pl.when(has[axis][0])
        def _():
            lo.wait_send()
            hi.wait_recv()

        @pl.when(has[axis][1])
        def _():
            hi.wait_send()
            lo.wait_recv()

    def field_copies(phase, u):
        s, w = snd.at[phase], rcv.at[phase]
        return (
            copies("gz", zs.at[phase], zr.at[phase, 1], zs.at[phase], zr.at[phase, 0], s, w),
            copies("gx", u.at[:, 1, 8:40, :], xr.at[phase, 1], u.at[:, 16, 8:40, :], xr.at[phase, 0], s, w),
            copies("gy", ys.at[phase, 0], yr.at[phase, 1], ys.at[phase, 1], yr.at[phase, 0], s, w),
        )

    def merged(low, high):
        return jnp.where(lane % 2 == 0, pltpu.roll(high, 127, 1), pltpu.roll(low, 1, 1))

    def ends_of(column, x):
        return jnp.concatenate([pltpu.roll(column, 127 - 8 * x - 2 * t, 1) for t in range(4)], axis=0)

    def along_z(centre, ends):
        up = jnp.where(lane32 == 127, ends, pltpu.roll(centre, 127, 1))
        down = jnp.where(lane32 == 0, ends, pltpu.roll(centre, 1, 1))
        return up, down

    def planes(body, carry=0, G=7):
        def step(i, carry):
            for j in range(G):
                carry = body(1 + i * G + j, carry)
            return carry
        return lax.fori_loop(0, 14 // G, step, carry)

    def pack_rows(phase, u):
        for comp in range(3):
            for x in range(16):
                ys[phase, 0, comp, x : x + 1, :] = u[comp, x + 1, 8:9, :]
                ys[phase, 1, comp, x : x + 1, :] = u[comp, x + 1, 39:40, :]

    def pack_ends(u):
        accs = [jnp.zeros((8, 128), F32) for _ in range(4)]
        for x in range(16):
            for t in range(4):
                i = 4 * x + t
                k = i % 4
                turned = pltpu.roll(u[x + 1, 8 * t + 8 : 8 * t + 16, :], 2 * i + 1, 1)
                accs[k] = jnp.where(lane // 2 == i, turned, accs[k])
        return (accs[0] + accs[1]) + (accs[2] + accs[3])

    def send_field(phase, u, x_sent=False):
        along_z, along_x, along_y = field_copies(phase, u)
        if not x_sent:
            start(along_x)
        pack_rows(phase, u)
        start(along_y)
        for comp in range(3):
            zs[phase, comp] = pack_ends(u.at[comp])
        start(along_z)
        return along_x, along_y, along_z

    load_u.wait()

    pl.semaphore_wait(barrier, len(lines) + len(plane) + has_across.astype(jnp.int32))
    sent = send_field(0, u0)

    for side, there in enumerate((gx == 0, gx == nx - 1)):
        @pl.when(there)
        def _(side=side):
            for phase in range(3):
                xr[phase, side] = jnp.zeros((3, 32, 128), F32)
            vxr[side] = jnp.zeros((32, 128), F32)
            cxr[side] = jnp.zeros((48, 128), F32)

    for side, there in enumerate((gy == 0, gy == ny - 1)):
        @pl.when(there)
        def _(side=side):
            for phase in range(3):
                yr[phase, side] = jnp.zeros((3, 16, 128), F32)
            vyr[side] = jnp.zeros((16, 128), F32)
            cyr[side] = jnp.zeros((24, 128), F32)

    for side, there in enumerate((gz == 0, gz == nz - 1)):
        @pl.when(there)
        def _(side=side):
            for phase in range(3):
                zr[phase, side] = jnp.zeros((3, 8, 128), F32)
            vzr[side] = jnp.zeros((8, 128), F32)
            czr[side] = jnp.zeros((8, 256), F32)

    for u in (u1, u2):
        for x in (0, 17):
            u[:, x, 8:40, :] = jnp.zeros((3, 32, 128), F32)
        u[:, :, 7:8, :] = jnp.zeros((3, 18, 1, 128), F32)
        u[:, :, 40:41, :] = jnp.zeros((3, 18, 1, 128), F32)
    for x in (0, 17):
        vis[x, 8:40, :] = jnp.zeros((32, 128), F32)
    vis[:, 7:8, :] = jnp.zeros((18, 1, 128), F32)
    vis[:, 40:41, :] = jnp.zeros((18, 1, 128), F32)

    ap[:, 0:8, :] = jnp.zeros((20, 8, 128), F32)
    ap[:, 40:48, :] = jnp.zeros((20, 8, 128), F32)
    t1[...] = jnp.zeros(t1.shape, F32)
    t2[...] = jnp.zeros(t2.shape, F32)

    load_phase.wait()
    load_pref.wait()
    load_yield.wait()
    blocks = phase_ref[...].reshape(32, 32)
    row = lax.broadcasted_iota(jnp.int32, (32, 128), 0)
    spread_z = (lane32 // 4 == row).astype(F32)
    r = lax.broadcasted_iota(jnp.int32, (128, 32), 0)
    c = lax.broadcasted_iota(jnp.int32, (128, 32), 1)
    spread_y = ((r // 32) * 8 + (r % 32) // 4 == c).astype(F32)
    for which, table in enumerate((pref_ref, yield_ref)):
        values = jnp.zeros((32, 32), F32)
        for phase in range(8):
            values = jnp.where(blocks == phase, table[phase], values)
        wide = jnp.dot(values, spread_z, precision=lax.Precision.HIGHEST, preferred_element_type=F32)
        cells[which] = jnp.dot(spread_y, wide, precision=lax.Precision.HIGHEST, preferred_element_type=F32)

    for pair in sent:
        wait(pair)
    for comp in range(3):
        u0[comp, 0, 8:40, :] = xr[0, 0, comp]
        u0[comp, 17, 8:40, :] = xr[0, 1, comp]
        for x in range(16):
            u0[comp, x + 1, 7:8, :] = yr[0, 0, comp, x : x + 1, :]
            u0[comp, x + 1, 40:41, :] = yr[0, 1, comp, x : x + 1, :]

    def inv_body(x, carry):
        d = []
        for comp in range(3):
            centre = u0[comp, x + 1, 8:40, :]
            up, down = along_z(centre, ends_of(ends[comp], x))
            d.append((
                u0[comp, x + 2, 8:40, :] - u0[comp, x, 8:40, :],
                u0[comp, x + 1, 9:41, :] - u0[comp, x + 1, 7:39, :],
                up - down,
            ))
        same = d[0][0] * d[0][0] + d[1][1] * d[1][1] + d[2][2] * d[2][2]
        xy, xz, yz = d[0][1] + d[1][0], d[0][2] + d[2][0], d[1][2] + d[2][1]
        off = xy * xy + xz * xz + yz * yz
        vis[x + 1, 8:40, :] = same * 0.125 + off * 0.0625 + 1.0
        return carry

    def law_body(x, carry):
        inv = vis[x + 1, 8:40, :]
        block = pl.ds((x // 4) * 32, 32)
        creep = cells[0, block, :] * jnp.exp(jnp.log(inv) * (-1.0 / 3.0))
        plastic = cells[1, block, :] * (0.5 * lax.rsqrt(inv))
        vis[x + 1, 8:40, :] = jnp.minimum(creep, plastic)
        return carry

    ends = [merged(zr[0, 0, comp], zr[0, 1, comp]) for comp in range(3)]
    vz = copies("gz", vzs, vzr.at[1], vzs, vzr.at[0], vsnd, vrcv)
    vx = copies("gx", vis.at[1, 8:40, :], vxr.at[1], vis.at[16, 8:40, :], vxr.at[0], vsnd, vrcv)
    vy = copies("gy", vys.at[0], vyr.at[1], vys.at[1], vyr.at[0], vsnd, vrcv)
    for body in (inv_body, law_body):
        body(0, 0)
        body(15, 0)
    start(vx)
    planes(inv_body, G=VG)
    planes(law_body, G=LG)
    for x in range(16):
        vys[0, x : x + 1, :] = vis[x + 1, 8:9, :]
        vys[1, x : x + 1, :] = vis[x + 1, 39:40, :]
    start(vy)
    vzs[...] = pack_ends(vis)
    start(vz)
    vsent = (vx, vy, vz)

    def everywhere(body, carry=0, G=7):
        return planes(body, body(15, body(0, carry)), G)

    flag = {a: tuple(jnp.where(h, 1.0, 0.0).astype(F32) for h in has[a]) for a in axes}

    def weighted(get, k, count):
        total = None
        for offset, weight in ((-1, 0.125), (0, 0.375), (1, 0.375), (2, 0.125)):
            i = 2 * k + offset
            if 0 <= i < count:
                term = get(i) * weight
                total = term if total is None else total + term
        return total

    at = 0
    prev = None
    for level, own in enumerate((8, 4, 2)):
        for k in range(-1, own + 1):
            if level == 0:
                value = weighted(lambda i: vis[i + 1, 8:40, :], k, 16)
            else:
                value = None
                for offset, weight in ((-1, 0.125), (0, 0.375), (1, 0.375), (2, 0.125)):
                    i = 2 * k + offset + 1
                    if 0 <= i < prev[1]:
                        term = ap[prev[0] + i, 8:40, :] * weight
                        value = term if value is None else value + term
            if k == -1:
                value = value * flag["gx"][0]
            if k == own:
                value = value * flag["gx"][1]
            ap[at + k + 1, 8:40, :] = value
        prev = (at, own + 2)
        at += own + 2

    def halve(src, start, rows):
        return (
            (src[:, pl.ds(5, rows, stride=2), :] + src[:, pl.ds(8, rows, stride=2), :])
            + 3.0 * (src[:, pl.ds(6, rows, stride=2), :] + src[:, pl.ds(7, rows, stride=2), :])
        ) * 0.125

    low_y, high_y = flag["gy"]
    t1[:, 7:25, :] = halve(ap, 5, 18)
    t1[:, 7:8, :] = t1[:, 7:8, :] * low_y
    t1[:, 24:25, :] = t1[:, 24:25, :] * high_y
    t2[:, 7:17, :] = halve(t1.at[10:20], 5, 10)
    t2[:, 7:8, :] = t2[:, 7:8, :] * low_y
    t2[:, 16:17, :] = t2[:, 16:17, :] * high_y
    t3[:, 7:13, :] = halve(t2.at[6:10], 5, 6)
    t3[:, 7:8, :] = t3[:, 7:8, :] * low_y
    t3[:, 12:13, :] = t3[:, 12:13, :] * high_y

    levels = ((t1, 0, 8, 16, 0, 0), (t2, 0, 4, 8, 24, 8), (t3, 0, 2, 4, 40, 16))
    for t, _, own, rows, at, _ in levels:
        cxs[0, at : at + rows + 2, :] = t[0, 7 : rows + 9, :]
        cxs[1, at : at + rows + 2, :] = t[own + 1, 7 : rows + 9, :]
    cx = copies("gx", cxs.at[0], cxr.at[1], cxs.at[1], cxr.at[0], csnd, crcv)
    start(cx)

    load_f.wait()
    ends_only = jnp.where((lane32 == 0) | (lane32 == 127), 0.5, 0.0).astype(F32)

    def face_body(x, carry):
        half = 0.5 * vis[x + 1, 8:40, :]
        faces = [
            half + 0.5 * vis[x, 8:40, :],
            half + 0.5 * vis[x + 2, 8:40, :],
            half + 0.5 * vis[x + 1, 7:39, :],
            half + 0.5 * vis[x + 1, 9:41, :],
            half + jnp.where(lane32 == 0, 0.0, pltpu.roll(half, 1, 1)),
            half + jnp.where(lane32 == 127, 0.0, pltpu.roll(half, 127, 1)),
        ]
        fx[x] = faces[0]
        fx[x + 1] = faces[1]
        fy[0, x] = faces[2]
        fy[1, x] = faces[3]
        fzl[x] = faces[4]
        fzh[x] = faces[5]
        diag[x] = ((faces[0] + faces[1]) + (faces[2] + faces[3])) + (faces[4] + faces[5])
        return carry

    def around(u, x, faces):
        total = faces[0] * u[x, 8:40, :] + faces[1] * u[x + 2, 8:40, :]
        return total + (faces[2] * u[x + 1, 7:39, :] + faces[3] * u[x + 1, 9:41, :])

    def faces_of(x):
        return [fx[x], fx[x + 1], fy[0, x], fy[1, x], fzl[x], fzh[x]]

    def first_base(x, carry):
        faces = faces_of(x)
        for comp in range(3):
            centre = u0[comp, x + 1, 8:40, :]
            up, down = along_z(centre, ends_of(ends[comp], x))
            total = around(u0.at[comp], x, faces) + (faces[4] * down + faces[5] * up)
            base[comp, x] = frc[comp, x] + total
        return carry

    everywhere(face_body)
    everywhere(first_base)

    for pair in vsent:
        wait(pair)
    vends = merged(vzr[0], vzr[1])

    def beside_y(row, side):
        return jnp.where(sub8 == (7 if side else 0), row, 0.0)

    def first_end(x, carry):
        extra_z = ends_only * ends_of(vends, x)
        extra = extra_z
        rows = [0.5 * beside_y(vyr[side, pl.ds(x, 1), :], side) for side in (0, 1)]
        nothing = jnp.zeros((16, 128), F32)
        extra = extra + jnp.concatenate([rows[0], nothing, rows[1]], axis=0)
        plane_x = None
        if isinstance(x, int) and x in (0, 15):
            side = x // 15
            plane_x = 0.5 * vxr[side]
            extra = extra + plane_x
        d = diag[x] + extra
        diag[x] = d
        s = RELAX / d
        scale[x] = s
        low, high = fzl[x], fzh[x]
        end = jnp.where(lane32 == 0, low, jnp.where(lane32 == 127, high, 0.0)) + extra_z
        fze[x] = end
        sz[x] = end * s
        fzl[x] = jnp.where(lane32 == 0, 0.0, low)
        fzh[x] = jnp.where(lane32 == 127, 0.0, high)
        low_y = fy[0, x, 0:8, :] + rows[0]
        high_y = fy[1, x, 24:32, :] + rows[1]
        fy[0, x, 0:8, :] = low_y
        fy[1, x, 24:32, :] = high_y
        sy[0, x] = jnp.where(sub8 == 0, low_y * s[0:8], 0.0)
        sy[1, x] = jnp.where(sub8 == 7, high_y * s[24:32], 0.0)
        if plane_x is not None:
            face = fx[x + side] + plane_x
            fx[x + side] = face
            sx[side] = face * s
        for comp in range(3):
            total = base[comp, x] + extra_z * ends_of(ends[comp], x)
            total = total + jnp.concatenate([
                rows[0] * row_of(0, 0, comp, x), nothing, rows[1] * row_of(0, 1, comp, x)], axis=0)
            if plane_x is not None:
                total = total + plane_x * xr[0, side, comp]
            u1[comp, x + 1, 8:40, :] = (1.0 - RELAX) * u0[comp, x + 1, 8:40, :] + s * total
        return carry

    def row_of(phase, side, comp, x):
        return yr[phase, side, comp, pl.ds(x, 1), :]

    def sweep_base(u, x):
        faces = faces_of(x)
        out = []
        for comp in range(3):
            centre = u[comp, x + 1, 8:40, :]
            total = around(u.at[comp], x, faces)
            total = total + (faces[4] * pltpu.roll(centre, 1, 1) + faces[5] * pltpu.roll(centre, 127, 1))
            out.append((centre, frc[comp, x] + total))
        return out

    def added(phase, ends, comp, x, value, z_face, y_faces, x_faces):
        value = value + z_face * ends_of(ends[comp], x)
        value = jnp.concatenate([
            value[0:8] + y_faces[0] * row_of(phase, 0, comp, x),
            value[8:24],
            value[24:32] + y_faces[1] * row_of(phase, 1, comp, x),
        ], axis=0)
        if isinstance(x, int) and x in (0, 15):
            value = value + x_faces[x // 15] * xr[phase, x // 15, comp]
        return value

    first_end(0, 0)
    first_end(15, 0)
    start(field_copies(1, u1)[1])
    planes(first_end, G=SG)
    sent = send_field(1, u1, True)

    wait(cx)
    for t, _, own, rows, at, _ in levels:
        t[1, 7 : rows + 9, :] = t[1, 7 : rows + 9, :] + cxr[0, at : at + rows + 2, :]
        t[own, 7 : rows + 9, :] = t[own, 7 : rows + 9, :] + cxr[1, at : at + rows + 2, :]
    for t, _, own, rows, _, at in levels:
        for k in range(own):
            cys[0, at + k : at + k + 1, :] = t[k + 1, 7:8, :]
            cys[1, at + k : at + k + 1, :] = t[k + 1, rows + 8 : rows + 9, :]
    cy = copies("gy", cys.at[0], cyr.at[1], cys.at[1], cyr.at[0], csnd, crcv)
    start(cy)

    def second_base(x, carry):
        s = scale[x]
        for comp, (centre, total) in enumerate(sweep_base(u1, x)):
            base[comp, x] = (1.0 - RELAX) * centre + s * total
        return carry

    everywhere(second_base)

    for pair in sent:
        wait(pair)
    ends1 = [merged(zr[1, 0, comp], zr[1, 1, comp]) for comp in range(3)]

    def second_end(x, carry):
        for comp in range(3):
            u2[comp, x + 1, 8:40, :] = added(
                1, ends1, comp, x, base[comp, x], sz[x], (sy[0, x], sy[1, x]), (sx[0], sx[1]))
        return carry

    second_end(0, 0)
    second_end(15, 0)
    start(field_copies(2, u2)[1])
    planes(second_end)
    sent = send_field(2, u2, True)

    wait(cy)
    at = 0
    for t, _, own, rows, _, place in levels:
        for k in range(own):
            value = t[k + 1, 8 : rows + 8, :]
            r = lax.broadcasted_iota(jnp.int32, (rows, 128), 0)
            value = value + jnp.where(r == 0, cyr[0, place + k : place + k + 1, :], 0.0)
            value = value + jnp.where(r == rows - 1, cyr[1, place + k : place + k + 1, :], 0.0)
            bc[at : at + rows, :] = value
            at += rows
    load_op.wait()
    load_sel.wait()
    czs[...] = jnp.zeros((8, 256), F32)
    czs[:, 0:168] = lax.dot_general(
        opm[128:136, :], bc[...], (((1,), (1,)), ((), ())),
        precision=lax.Precision.HIGHEST, preferred_element_type=F32)
    cz = copies("gz", czs, czr.at[1], czs, czr.at[0], csnd, crcv)
    start(cz)

    def resid_base(x, carry):
        d = diag[x]
        for comp, (centre, total) in enumerate(sweep_base(u2, x)):
            base[comp, x] = total - d * centre
        return carry

    everywhere(resid_base)

    for pair in sent:
        wait(pair)
    ends2 = [merged(zr[2, 0, comp], zr[2, 1, comp]) for comp in range(3)]

    def resid_end(x, acc):
        low_y = jnp.where(sub8 == 0, fy[0, x, 0:8, :], 0.0)
        high_y = jnp.where(sub8 == 7, fy[1, x, 24:32, :], 0.0)
        for comp in range(3):
            left = added(2, ends2, comp, x, base[comp, x], fze[x], (low_y, high_y), (fx[0], fx[16]))
            res[comp, x] = left
            square = left * left
            acc = acc + ((square[0:8] + square[8:16]) + (square[16:24] + square[24:32]))
        return acc

    acc = everywhere(resid_end, jnp.zeros((8, 128), F32))

    place = core * nz + gz
    ar_a[place] = jnp.sum(acc, axis=0, keepdims=True)
    for px, pz in lines:
        pltpu.make_async_remote_copy(
            ar_a.at[place], ar_a.at[place], asnd.at[0], arcv.at[0],
            device_id={"gx": px, "gz": pz}, device_id_type=MESH).start()

    wait(cz)
    got = jnp.concatenate([czr[0], czr[1]], axis=0)[:, 0:168]
    coarse = jnp.dot(bc[...], opm[0:128, :], precision=lax.Precision.HIGHEST, preferred_element_type=F32)
    coarse = coarse + lax.dot_general(
        got, sel_ref[...], (((0,), (0,)), ((), ())),
        precision=lax.Precision.HIGHEST, preferred_element_type=F32)
    c1_ref[...] = coarse[0:128, 0:64].reshape(8, 16, 64)
    c2_ref[...] = coarse[128:160, 64:96].reshape(4, 8, 32)
    c3_ref[0] = coarse[160:164, 96:112]
    c3_ref[1] = coarse[164:168, 96:112]

    def whole(buf, n, sem):
        return pltpu.make_async_copy(buf.at[0:n], buf.at[0:n], sem)

    whole(ar_a, len(lines), asnd.at[0]).wait()
    whole(ar_a, len(lines), arcv.at[0]).wait()
    mine = chip * ny + gy
    ar_b[mine] = jnp.sum(ar_a[...], axis=0)
    for px, py in plane:
        pltpu.make_async_remote_copy(
            ar_b.at[mine], ar_b.at[mine], asnd.at[1], arcv.at[1],
            device_id={"gx": px, "gy": py}, device_id_type=MESH).start()
    whole(ar_b, len(plane), asnd.at[1]).wait()
    whole(ar_b, len(plane), arcv.at[1]).wait()
    total = jnp.sum(ar_b[...], axis=0)
    cells_all = float(3 * 16 * nx * 32 * ny * 128 * nz)
    rms_ref[...] = jnp.sqrt(jnp.sum(total, axis=1, keepdims=True) / cells_all)


def store(u2, vis, c1, c2, c3, res, rms, smooth_hbm, visc_hbm, c1_hbm, c2_hbm, c3_hbm, resid_hbm, rms_hbm, sem):
    pairs = [(u2.at[comp, x + 1 : x + 9, 8:40, :], smooth_hbm.at[comp, x : x + 8]) for comp in range(3) for x in (0, 8)]
    pairs += [(res.at[comp, x : x + 8], resid_hbm.at[comp, x : x + 8]) for comp in range(3) for x in (0, 8)]
    pairs += [(vis.at[x + 1 : x + 9, 8:40, :], visc_hbm.at[x : x + 8]) for x in (0, 8)]
    pairs += [(c1, c1_hbm), (c2, c2_hbm), (c3, c3_hbm), (rms, rms_hbm)]
    copies = [pltpu.make_async_copy(a, b, sem.at[i]) for i, (a, b) in enumerate(pairs)]
    for copy in copies:
        copy.start()
    for copy in copies:
        copy.wait()


def per_device(sizes, velocity, forcing, phase_block, prefactor, yield_stress):
    nx, ny, nz = sizes
    vm = lambda *shape: pltpu.VMEM(shape, F32)
    any_, hbm, vmem = (pl.BlockSpec(memory_space=s) for s in (pl.ANY, pltpu.HBM, pltpu.VMEM))
    shape = lambda *s: jax.ShapeDtypeStruct(s, F32)
    out = pl.pallas_call(
        functools.partial(kernel, sizes),
        out_shape=(
            vm(3, 18, 48, 128), vm(18, 48, 128), vm(8, 16, 64), vm(4, 8, 32), vm(2, 4, 16),
            vm(3, 16, 32, 128), vm(1, 1),
        ),
        in_specs=[hbm] * 7,
        out_specs=(vmem,) * 7,
        scratch_shapes=[
            vm(3, 18, 48, 128), vm(3, 18, 48, 128), vm(3, 16, 32, 128),
            vm(17, 32, 128), vm(2, 16, 32, 128), vm(16, 32, 128), vm(16, 32, 128), vm(16, 32, 128),
            vm(16, 32, 128), vm(16, 32, 128), vm(3, 16, 32, 128), vm(2, 32, 128), vm(2, 16, 8, 128), vm(16, 32, 128),
            vm(2, 128, 128), vm(3, 2, 3, 32, 128), vm(3, 2, 3, 16, 128), vm(3, 2, 3, 16, 128), vm(3, 2, 3, 8, 128), vm(3, 3, 8, 128),
            vm(2, 32, 128), vm(2, 16, 128), vm(2, 16, 128), vm(2, 8, 128), vm(8, 128),
            vm(20, 48, 128), vm(20, 32, 128), vm(10, 24, 128), vm(4, 16, 128),
            vm(2, 48, 128), vm(2, 48, 128), vm(2, 24, 128), vm(2, 24, 128), vm(8, 256), vm(2, 8, 256),
            vm(168, 128), vm(136, 128),
            vm(2 * nz, 1, 128), vm(nx // 2 * ny, 1, 128),
            pltpu.VMEM((4, 8, 32), jnp.int32), vm(16, 128), pltpu.SMEM((8,), F32), pltpu.SMEM((8,), F32),
            pltpu.SemaphoreType.DMA((7,)),
            pltpu.SemaphoreType.DMA((3, 3, 2)), pltpu.SemaphoreType.DMA((3, 3, 2)),
            pltpu.SemaphoreType.DMA((3, 2)), pltpu.SemaphoreType.DMA((3, 2)),
            pltpu.SemaphoreType.DMA((3, 2)), pltpu.SemaphoreType.DMA((3, 2)),
            pltpu.SemaphoreType.DMA((2,)), pltpu.SemaphoreType.DMA((2,)),
        ],
        compiler_params=pltpu.CompilerParams(collective_id=0, has_side_effects=True, vmem_limit_bytes=60 << 20),
        name="picard",
    )(
        velocity, forcing, phase_block, jnp.asarray(depth_operator()), jnp.asarray(depth_places()),
        prefactor, yield_stress,
    )
    out = pl.pallas_call(
        store,
        out_shape=(
            shape(3, 16, 32, 128), shape(16, 32, 128), shape(8, 16, 64), shape(4, 8, 32), shape(2, 4, 16),
            shape(3, 16, 32, 128), shape(1, 1),
        ),
        in_specs=[vmem] * 7,
        out_specs=(any_,) * 7,
        scratch_shapes=[pltpu.SemaphoreType.DMA((18,))],
        compiler_params=pltpu.CompilerParams(vmem_limit_bytes=1 << 20),
        name="store",
    )(*out)
    return out[:6] + (out[6].reshape(()),)


def solution(mesh):
    sizes = tuple(mesh.shape[a] for a in ("gx", "gy", "gz"))
    return jax.shard_map(
        functools.partial(per_device, sizes),
        mesh=mesh,
        in_specs=(P(None, "gx", "gy", "gz"), P(None, "gx", "gy", "gz"), P("gx", "gy", "gz"), P(), P()),
        out_specs=(
            P(None, "gx", "gy", "gz"), P("gx", "gy", "gz"), P("gx", "gy", "gz"), P("gx", "gy", "gz"),
            P("gx", "gy", "gz"), P(None, "gx", "gy", "gz"), P(),
        ),
        check_vma=False,
    )
```
